128 devices in a mesh: gx: 8 (over z, x_lo), gy: 16 (over y, x_hi, core).
Axes of the slice: x: 4 (x_hi: 2, x_lo: 2; x = x_hi * 2 + x_lo), y: 4, z: 4, core: 2. Of those that a mesh axis runs over, the one named last changes fastest.
Arguments:
- x_gen: bfloat16 [16, 1024, 3072], P('gy', 'gx'), may hold values from -6 to 6
- fresh_noise: bfloat16 [16, 1024, 3072], P('gy', 'gx'), may hold values from -6 to 6
- steps_t: int32 [16], P('gy'), may hold values from 0 to 999
- real_mod: float32 [16, 2, 3072], P('gy'), may hold values from -2.5 to 2.5
- real_w_up: bfloat16 [3072, 6144], P(None, 'gx'), may hold values from -0.109375 to 0.109375
- real_b_up: float32 [6144], P('gx'), may hold values from -3 to 3
- real_w_down: bfloat16 [6144, 3072], P('gx'), may hold values from -0.078125 to 0.078125
- fake_mod: float32 [16, 2, 3072], P('gy'), may hold values from -2.5 to 2.5
- fake_w_up: bfloat16 [3072, 6144], P('gy', 'gx'), may hold values from -0.109375 to 0.109375
- fake_b_up: float32 [6144], P('gx'), may hold values from -3 to 3
- fake_w_down: bfloat16 [6144, 3072], P('gx', 'gy'), may hold values from -0.078125 to 0.078125
Outputs:
- dmd_grad: float32 [16, 1024, 3072], P('gy', 'gx')
- fake_grad: float32 [3072, 6144], P('gy', 'gx')
The draws below stay inside these ranges and needn't reach their ends.
All inputs are finite; a program needn't handle non-finite values.
Results may differ from the reference program's by a relative error of at most 0.013.
Values may be sent and summed in bfloat16 or wider, within the bound.
No kernel may reach another device: no remote copies, remote signals or barrier semaphores. Data moves between devices by JAX's collectives and lax.ppermute only.
A program may use at most 128 MiB of HBM per device.

```python
import jax
import jax.numpy as jnp
from jax import lax

D = 3072
FF = 6144
TSTEPS = 1000
SEQ = 1024
SAMPLES = 16
N_GX = 8
N_GY = 16


def set_ends(entries, rng, smallest, high):
    spot = [jax.random.randint(jax.random.fold_in(rng, axis), (), 0, length) for axis, length in enumerate(entries.shape)]
    main_axis = entries.shape.index(max(entries.shape))
    neighbour = spot[:main_axis] + [(spot[main_axis] + 1) % entries.shape[main_axis]] + spot[main_axis + 1:]
    return entries.at[tuple(spot)].set(smallest).at[tuple(neighbour)].set(high)


def level_of(key, dims, cuts, least, top_value):
    def one(axis_at, blocks):
        draws = jax.random.uniform(jax.random.fold_in(jax.random.fold_in(key, 6), axis_at), (blocks,), jnp.float32, least / len(cuts), top_value / len(cuts))
        return jnp.repeat(jnp.exp(draws), dims[axis_at] // blocks).reshape((-1,) + (1,) * (len(dims) - axis_at - 1))

    factor_of = one(*cuts[0])
    for cut in cuts[1:]:
        factor_of = factor_of * one(*cut)
    return factor_of


def normal_values(own_key, dims, scale, reach, shards=(), dtype=jnp.bfloat16):
    array = jax.random.normal(own_key, dims, jnp.float32) * scale
    if len(shards) > 0:
        array = level_of(own_key, dims, shards, -0.22, 0.18) * array
    return jnp.clip(array, min=-reach, max=reach).astype(dtype)


def setup_inputs(seed: int = 0) -> dict:
    seeds = jax.random.split(jax.random.key(seed), 12)
    return {
        "x_gen": normal_values(seeds[0], (SAMPLES, SEQ, D), 1.0, 6.0, ((0, 16), (1, 8))),
        "fresh_noise": normal_values(seeds[1], (SAMPLES, SEQ, D), 1.0, 6.0, ((0, 16), (1, 8))),
        "steps_t": set_ends(jax.random.randint(seeds[2], (SAMPLES,), 0, TSTEPS), jax.random.fold_in(seeds[2], 1), 0, TSTEPS - 1).astype(jnp.int32),
        "real_mod": normal_values(seeds[3], (SAMPLES, 2, D), 0.3, 2.5, ((0, 16),), jnp.float32),
        "real_w_up": normal_values(seeds[4], (D, FF), D ** -0.5, 0.109375, ((1, 8),)),
        "real_b_up": normal_values(seeds[5], (FF,), 0.5, 3.0, ((0, 8),), jnp.float32),
        "real_w_down": normal_values(seeds[6], (FF, D), FF ** -0.5, 0.078125, ((0, 8),)),
        "fake_mod": normal_values(seeds[7], (SAMPLES, 2, D), 0.3, 2.5, ((0, 16),), jnp.float32),
        "fake_w_up": normal_values(seeds[8], (D, FF), D ** -0.5, 0.109375, ((0, 16), (1, 8))),
        "fake_b_up": normal_values(seeds[9], (FF,), 0.5, 3.0, ((0, 8),), jnp.float32),
        "fake_w_down": normal_values(seeds[10], (FF, D), FF ** -0.5, 0.078125, ((0, 8), (1, 16))),
    }


def layer_norm(values):
    center = values - lax.optimization_barrier(jnp.mean(values, axis=-1, keepdims=True))
    spread = lax.optimization_barrier(jnp.mean(center * center, axis=-1, keepdims=True))
    return center * lax.rsqrt(spread + 1e-06)

def net_pred(normed, modulation, w_up, b_up, w_down):
    modulated = (normed * (1.0 + modulation[1]) + modulation[0]).astype(jnp.bfloat16)
    hidden = jax.nn.gelu(jnp.dot(modulated, w_up, preferred_element_type=jnp.float32) + b_up, approximate=True).astype(jnp.bfloat16)
    group_size = FF // N_GX
    partials = jnp.einsum('sgk,gkd->gsd', hidden.reshape(SEQ, N_GX, group_size).astype(jnp.float32), w_down.reshape(N_GX, group_size, D).astype(jnp.float32))
    partials = lax.optimization_barrier(partials.astype(jnp.bfloat16)).astype(jnp.float32)
    return (lax.optimization_barrier(jnp.sum(partials, axis=0)), hidden)

def reference(x_gen, fresh_noise, steps_t, real_mod, real_w_up, real_b_up, real_w_down, fake_mod, fake_w_up, fake_b_up, fake_w_down):
    loss_scale = float(SEQ * N_GY) ** (-0.5)

    def per_sample(grad_total, inputs):
        clean, drawn, step_index, modulation_real, modulation_fake = inputs
        noise_level = (step_index.astype(jnp.float32) + 1.0) / TSTEPS
        clean_f = clean.astype(jnp.float32)
        drawn_f = drawn.astype(jnp.float32)
        noised = ((1.0 - noise_level) * clean_f + noise_level * drawn_f).astype(jnp.bfloat16)
        target = (drawn_f - clean_f).astype(jnp.bfloat16)
        normed = layer_norm(noised.astype(jnp.float32))
        pred_real, unused_hidden = net_pred(normed, modulation_real, real_w_up, real_b_up, real_w_down)
        pred_fake, hidden_fake = net_pred(normed, modulation_fake, fake_w_up, fake_b_up, fake_w_down)
        dmd_grad = pred_fake - pred_real
        error_v = (pred_fake - target.astype(jnp.float32)).astype(jnp.bfloat16)
        partial_term = jnp.dot(error_v.T, hidden_fake, preferred_element_type=jnp.float32) * loss_scale
        partial_term = lax.optimization_barrier(partial_term.astype(jnp.bfloat16)).astype(jnp.float32)
        return (grad_total + partial_term, dmd_grad)
    grad_start = jnp.zeros((D, FF), jnp.float32)
    fake_grad, dmd_grad = lax.scan(per_sample, grad_start, (x_gen, fresh_noise, steps_t, real_mod, fake_mod))
    return (dmd_grad, fake_grad)
```

```python
import jax
import jax.numpy as jnp
from jax import lax
from jax.sharding import Mesh
from jax.sharding import PartitionSpec as P

TSTEPS = 1000
GX = ("z", "p")
GY = ("y", "h", "c")
CHUNKS = 2
BF = jnp.bfloat16
F32 = jnp.float32


def turn(array, axis, step):
    n = lax.axis_size(axis)
    return lax.ppermute(array, axis, [(i, (i + step) % n) for i in range(n)])


def along_x(array, moves):
    place = (0, 2, 1, 3)
    return lax.ppermute(array, ("p", "h"), [(place[i], place[j]) for i, j in moves])


def z_gather(block):
    half = block.shape[0] // 2
    below = turn(block, "z", 1)
    above = turn(block, "z", -1)
    far_0 = turn(below[:half], "z", 1)
    far_1 = turn(above[half:], "z", -1)
    return jnp.concatenate([block, below, above, far_0, far_1], axis=0)


def z_scatter(part):
    n = part.shape[0] // 4
    half = n // 2
    own, below, above, far = (part[i * n : (i + 1) * n] for i in range(4))
    relay_0 = turn(far[:half].astype(BF), "z", 1).astype(F32)
    relay_1 = turn(far[half:].astype(BF), "z", -1).astype(F32)
    up_1 = turn(above[half:].astype(BF), "z", 1)
    down_0 = turn(below[:half].astype(BF), "z", -1)
    up_0 = turn((above[:half] + relay_0).astype(BF), "z", 1)
    down_1 = turn((below[half:] + relay_1).astype(BF), "z", -1)
    first = own[:half] + up_0.astype(F32) + down_0.astype(F32)
    second = own[half:] + up_1.astype(F32) + down_1.astype(F32)
    return jnp.concatenate([first, second], axis=0)


def half_of(array, k):
    lead = array.shape[:-1]
    cut = array.reshape(lead + (4, 2, array.shape[-1] // 8))
    picked = lax.dynamic_index_in_dim(cut, k, axis=len(lead) + 1, keepdims=False)
    return picked.reshape(lead + (array.shape[-1] // 2,))


def in_order(mine, other, p):
    return jnp.concatenate(
        [jnp.where(p == 0, mine, other), jnp.where(p == 0, other, mine)], axis=0
    )


def layer_norm(values):
    center = values - jnp.mean(values, axis=-1, keepdims=True)
    spread = jnp.mean(center * center, axis=-1, keepdims=True)
    return center * lax.rsqrt(spread + 1e-06)


def modulate(normed, modulation):
    return (normed * (1.0 + modulation[1]) + modulation[0]).astype(BF)


def dot_t(a, b, dims):
    return lax.dot_general(a, b, ((dims[:1], dims[1:]), ((), ())), preferred_element_type=F32)


def shards(
    x_gen,
    fresh_noise,
    steps_t,
    real_mod,
    real_w_up,
    real_b_up,
    real_w_down,
    fake_mod,
    fake_w_up,
    fake_b_up,
    fake_w_down,
):
    p, h, c = lax.axis_index("p"), lax.axis_index("h"), lax.axis_index("c")
    noise_level = (steps_t[0].astype(F32) + 1.0) / TSTEPS
    clean_f = x_gen[0].astype(F32)
    drawn_f = fresh_noise[0].astype(F32)
    noised = ((1.0 - noise_level) * clean_f + noise_level * drawn_f).astype(BF)
    target = (drawn_f - clean_f).astype(BF)
    own_rows = noised.shape[0]
    rows = own_rows // CHUNKS

    chunks = []
    for i in range(CHUNKS):
        mine = noised[i * rows : (i + 1) * rows]
        pair = in_order(mine, turn(mine, "p", 1), p)
        chunks.append(z_gather(pair))

    w_up = lax.all_gather(fake_w_up, GY, axis=0, tiled=True)
    block = fake_w_down.T
    from_a = along_x(block, [(0, 2), (3, 1)])
    from_b = along_x(block, [(1, 0), (2, 3)])
    from_c = along_x(block, [(1, 2), (2, 1)])
    both = jnp.concatenate(
        [jnp.where(h == p, block, from_a), jnp.where(h == p, from_b, from_c)], axis=1
    )
    w_down = lax.all_gather(both, ("y", "c"), axis=0, tiled=True)

    target_mine = half_of(target, p)
    target_other = turn(half_of(target, 1 - p), "p", 1)

    half_rows = real_w_down.shape[0] // 2
    given = half_of(lax.dynamic_slice_in_dim(real_w_down, c * half_rows, half_rows, axis=0), 1 - p)
    taken = turn(given, "p", 1)
    taken = in_order(taken, turn(taken, "c", 1), c)
    real_down = jnp.concatenate([half_of(real_w_down, p), taken], axis=0)

    def hidden(chunk, modulation, up, bias):
        pre = jnp.dot(modulate(layer_norm(chunk.astype(F32)), modulation), up, preferred_element_type=F32)
        own = jax.nn.gelu(pre + bias, approximate=True).astype(BF)
        return jnp.concatenate([own, turn(own, "p", 1)], axis=1)

    fake_hidden = [hidden(k, fake_mod[0], w_up, fake_b_up) for k in chunks]
    real_hidden = [hidden(k, real_mod[0], real_w_up, real_b_up) for k in chunks]

    fakes, product = [], None
    for i in range(CHUNKS):
        cut = slice(i * rows, (i + 1) * rows)
        fake_rows = z_scatter(dot_t(fake_hidden[i], w_down, (1, 1)))
        fakes.append(fake_rows)
        wanted = in_order(target_mine[cut], target_other[cut], p)
        error = z_gather((fake_rows - wanted.astype(F32)).astype(BF))
        part = dot_t(error, fake_hidden[i], (0, 0))
        product = part if product is None else product + part

    loss_scale = float(lax.axis_size(GY) * lax.axis_size(GX) * own_rows) ** (-0.5)
    width = fake_w_down.shape[1]
    cut_product = (product * loss_scale).reshape(4, 2, width, product.shape[1])
    kept = lax.dynamic_index_in_dim(cut_product, c, axis=1, keepdims=False)
    sent = lax.dynamic_index_in_dim(cut_product, 1 - c, axis=1, keepdims=False).astype(BF)
    summed = (kept + turn(sent, "c", 1).astype(F32)).astype(BF)
    summed = lax.all_to_all(summed, "y", 0, 0, tiled=True)
    summed = jnp.sum(summed.astype(F32), axis=0)
    n_hidden = summed.shape[1] // 2
    own_part, other_part = summed[:, :n_hidden], summed[:, n_hidden:].astype(BF)
    got_a = along_x(own_part.astype(BF), [(2, 0), (1, 3)]).astype(F32)
    got_b = along_x(other_part, [(0, 1), (3, 2)]).astype(F32)
    got_c = along_x(other_part, [(1, 2), (2, 1)]).astype(F32)
    fake_grad = jnp.where(h == p, own_part + got_a, got_b + got_c)

    outs = []
    for i in range(CHUNKS):
        real_rows = z_scatter(jnp.dot(real_hidden[i], real_down, preferred_element_type=F32))
        diff = fakes[i] - real_rows
        mine = lax.dynamic_slice_in_dim(diff, p * rows, rows, axis=0)
        other = lax.dynamic_slice_in_dim(diff, (1 - p) * rows, rows, axis=0).astype(BF)
        other = turn(other, "p", 1).astype(F32)
        mine, other = (v.reshape(rows, 4, 1, v.shape[1] // 4) for v in (mine, other))
        whole = jnp.concatenate(
            [jnp.where(p == 0, mine, other), jnp.where(p == 0, other, mine)], axis=2
        )
        outs.append(whole.reshape(rows, -1))
    return (jnp.concatenate(outs, axis=0)[None], fake_grad)


def solution(mesh):
    finer = Mesh(mesh.devices.reshape(4, 2, 4, 2, 2), GX + GY)
    placed = (
        P(GY, GX, None),
        P(GY, GX, None),
        P(GY),
        P(GY, None, None),
        P(None, GX),
        P(GX),
        P(GX, None),
        P(GY, None, None),
        P(GY, GX),
        P(GX),
        P(GX, GY),
    )
    return jax.shard_map(
        shards,
        mesh=finer,
        in_specs=placed,
        out_specs=(P(GY, GX, None), P(GY, GX)),
        check_vma=False,
    )
```
